32 devices in a mesh: shadow: 16 (over z, y, core), vocab: 2 (over x).
Axes of the slice: x: 2, y: 2, z: 4, core: 2. Of those that a mesh axis runs over, the one named last changes fastest.
Arguments:
- hidden: bfloat16 [64, 128, 2048], P('shadow'), may hold values from -18 to 18
- targets: int32 [128], replicated, may hold values from 0 to 4095
- membership: int32 [64, 4], P('shadow'), may hold values from 0 to 1, as said below
- unembedding: bfloat16 [4096, 2048], P(('shadow', 'vocab')), may hold values from -1 to 1
Outputs:
- score: float32 [64, 128], P('shadow', 'vocab')
The draws below stay inside these ranges and needn't reach their ends.
Inputs may be any that keep to these rules, and one draw needn't show every extreme that they name: `membership`: each candidate sequence is a member of exactly 32 of the shadow models.
All inputs are finite; a program needn't handle non-finite values.
Results may differ from the reference program's by a relative error of at most 0.00055.
Values may be sent and summed in bfloat16 or wider, within the bound.
A program may use at most 64 MiB of HBM per device.

```python
import math
import jax
import jax.numpy as jnp
import numpy as np
from jax import lax

D = 2048
TOK = 128
SEQ = 32
SHADOWS = 64
VOCAB = 4096
EXAMPLES = 4


def head_table(key):
    unscaled = jax.random.truncated_normal(jax.random.fold_in(key, 11), -4.0, 4.0, (VOCAB, D), jnp.float32)
    return unscaled * D ** (-0.5)


def draw_unembedding(key, part):
    return head_table(key).astype(jnp.bfloat16)


def draw_hidden(key, part):
    states = jnp.clip(jax.random.normal(jax.random.fold_in(key, 12), (SHADOWS, TOK, D), jnp.float32), -4.0, 4.0)
    return states.astype(jnp.bfloat16)


def draw_membership(key, part):
    noise = jax.random.randint(jax.random.fold_in(key, 13), (SHADOWS, EXAMPLES), 0, 1 << 20, jnp.int32)
    noise = noise * SHADOWS + jnp.arange(SHADOWS, dtype=jnp.int32)[:, None]
    ordering = jnp.argsort(noise, axis=0)
    ranking = jnp.argsort(ordering, axis=0)
    return (ranking < SHADOWS // 2).astype(jnp.int32)


def touch_ends(array, own_key, low, high):
    longest = array.shape.index(max(array.shape))
    spots = []
    for shift in (0, 1):
        where = [jax.random.randint(jax.random.fold_in(own_key, axis), (), 0, length) for axis, length in enumerate(array.shape)]
        where[longest] = (where[longest] + shift) % array.shape[longest]
        spots.append(tuple(where))
    return array.at[spots[0]].set(low).at[spots[1]].set(high)


def cumulative_ranks(number_of, lean):
    loads = [(1 << 20) // math.isqrt(standing ** lean) + 1 for standing in range(1, number_of + 1)]
    spread = 1 + sum(loads) // (1 << 30)
    return np.cumsum(np.array([max(1, weight // spread) for weight in loads]))


def skewed_ids(key, shape, amount, skew):
    grid = cumulative_ranks(amount, skew)
    ticket = jax.random.randint(jax.random.fold_in(key, 1), shape, 0, int(grid[amount - 1]))
    rank = jnp.searchsorted(jnp.asarray(grid, jnp.int32), ticket, side="right")
    return jax.random.permutation(jax.random.fold_in(key, 2), amount)[rank].astype(jnp.int32)


def setup_inputs(seed: int = 0) -> dict:
    keys = jax.random.split(jax.random.key(seed), 5)
    hidden = draw_hidden(jax.random.fold_in(keys[4], 71), 0)
    targets = touch_ends(skewed_ids(keys[1], (TOK,), VOCAB, 2), jax.random.fold_in(keys[1], 3), 0, VOCAB - 1).astype(jnp.int32)
    membership = draw_membership(jax.random.fold_in(keys[4], 71), 0)
    unembedding = draw_unembedding(jax.random.fold_in(keys[4], 71), 0)
    return dict(hidden=hidden, targets=targets, membership=membership, unembedding=unembedding)


NEG_FILL = -1e+30
VAR_FLOOR = 0.5

def reference(hidden, targets, membership, unembedding):
    columns = jnp.arange(unembedding.shape[0], dtype=jnp.int32)
    target_hit = targets.astype(jnp.int32)[:, None] == columns[None, :]

    def confidence_of(states):
        logits = lax.dot_general(states, unembedding, (((1,), (1,)), ((), ())), preferred_element_type=jnp.float32)
        target_logit = lax.optimization_barrier(jnp.sum(jnp.where(target_hit, logits, 0.0), axis=1))
        others = jnp.where(target_hit, NEG_FILL, logits)
        highest = lax.optimization_barrier(jnp.max(others, axis=1))
        summed = lax.optimization_barrier(jnp.sum(jnp.where(target_hit, 0.0, jnp.exp(others - highest[:, None])), axis=1))
        return target_logit - (highest + jnp.log(summed))
    confidence = lax.map(confidence_of, hidden)
    outside = (1 - jnp.repeat(membership, SEQ, axis=1)).astype(jnp.float32)
    weighted = outside * confidence
    first_moment = lax.optimization_barrier(jnp.sum(weighted, axis=0))
    second_moment = lax.optimization_barrier(jnp.sum(weighted * confidence, axis=0))
    out_count = SHADOWS // 2 - outside
    out_mean = (first_moment[None, :] - weighted) / out_count
    out_variance = (second_moment[None, :] - weighted * confidence) / out_count - out_mean * out_mean
    return (confidence - out_mean) * lax.rsqrt(jnp.maximum(out_variance, 0.0) + VAR_FLOOR)
```

```python
import functools

import jax
import jax.numpy as jnp
from jax import lax
from jax.experimental import pallas as pl
from jax.experimental.pallas import tpu as pltpu
from jax.sharding import PartitionSpec as P

SEQ = 32
NEG_FILL = -1e30
VAR_FLOOR = 0.5
MESH = pl.DeviceIdType.MESH

HEAD_CHUNKS = 4
HIDDEN_CHUNKS = 8


def kernel(
    nsh,
    nv,
    seq,
    hidden_hbm,
    targets_hbm,
    member_hbm,
    head_hbm,
    out_ref,
    targets_ref,
    member_ref,
    hid,
    heads,
    top,
    tot,
    tgt,
    acc,
    outs,
    stat_send,
    stat_recv,
    mom_send,
    mom_recv,
    load_sem,
    line_send,
    line_recv,
    sib_send,
    sib_recv,
    hy_send,
    hy_recv,
    hx_send,
    hx_recv,
    st_send,
    st_recv,
    mo_send,
    mo_recv,
    ou_send,
    ou_recv,
):
    nz = nsh // 4
    chunks, head_rows, slab = heads.shape[1], heads.shape[2], heads.shape[3]
    rows = hid.shape[1]
    tokens = targets_ref.shape[1]
    group = rows // tokens
    piece = rows // nv
    hparts = hy_recv.shape[0]
    part = piece // hparts

    me = lax.axis_index("shadow")
    v = lax.axis_index("vocab")
    z, y, c = me // 4, (me // 2) % 2, me % 2
    sibling = me + 1 - 2 * c
    across = me + 2 - 4 * y
    has_up, has_down = z + 1 < nz, z >= 1
    one, zero = jnp.int32(1), jnp.int32(0)
    last = nz - 1
    at_end = (z == 0) | (z == last)
    final = jnp.where(z == 0, jnp.int32(last), zero)

    load_head = [
        pltpu.make_async_copy(
            head_hbm.at[:, pl.ds(j * slab, slab)], heads.at[2 * z + c, j], load_sem.at[j]
        )
        for j in range(chunks)
    ]
    load_hidden = pltpu.make_async_copy(hidden_hbm, hid.at[0], load_sem.at[chunks])
    load_small = [
        pltpu.make_async_copy(targets_hbm, targets_ref, load_sem.at[chunks + 1]),
        pltpu.make_async_copy(member_hbm, member_ref, load_sem.at[chunks + 2]),
    ]
    for copy in load_head + [load_hidden] + load_small:
        copy.start()

    barrier = pltpu.get_barrier_semaphore()

    def greet(s, w):
        pl.semaphore_signal(barrier, inc=1, device_id=(s, w), device_id_type=MESH)

    greet(sibling, v)
    greet(across, v)
    for d in range(1, nv):
        greet(me, (v + d) % nv)

    @pl.when(has_up)
    def _():
        greet(me + 4, v)

    @pl.when(has_down)
    def _():
        greet(me - 4, v)

    top[...] = jnp.full_like(top, NEG_FILL)
    tot[...] = jnp.zeros_like(tot)
    tgt[...] = jnp.zeros_like(tgt)
    pl.semaphore_wait(
        barrier, nv + 1 + jnp.where(has_up, one, zero) + jnp.where(has_down, one, zero)
    )

    def line(block, j, target):
        return pltpu.make_async_remote_copy(
            src_ref=heads.at[2 * block + c, j],
            dst_ref=heads.at[2 * block + c, j],
            send_sem=line_send.at[0],
            recv_sem=line_recv.at[block, j],
            device_id=(target, v),
            device_id_type=MESH,
        )

    def side(block, j, core):
        return pltpu.make_async_remote_copy(
            src_ref=heads.at[2 * block + core, j],
            dst_ref=heads.at[2 * block + core, j],
            send_sem=sib_send.at[0],
            recv_sem=sib_recv.at[jnp.where(at_end & (block == final), nz + j, block)],
            device_id=(sibling, v),
            device_id_type=MESH,
        )

    def over_y(i):
        where = pl.ds(pl.multiple_of(v * piece + i * part, part), part)
        return pltpu.make_async_remote_copy(
            src_ref=hid.at[0, where],
            dst_ref=hid.at[1, where],
            send_sem=hy_send.at[0],
            recv_sem=hy_recv.at[i],
            device_id=(across, v),
            device_id_type=MESH,
        )

    def over_x(d, i, owner):
        where = pl.ds(pl.multiple_of(owner * piece + i * part, part), part)
        return pltpu.make_async_remote_copy(
            src_ref=hid.at[1, where],
            dst_ref=hid.at[1, where],
            send_sem=hx_send.at[0],
            recv_sem=hx_recv.at[d - 1],
            device_id=(me, (v + d) % nv),
            device_id_type=MESH,
        )

    for j in range(chunks):
        load_head[j].wait()

        @pl.when(has_up)
        def _():
            line(z, j, me + 4).start()

        @pl.when(has_down)
        def _():
            line(z, j, me - 4).start()

        side(z, j, c).start()
    load_hidden.wait()
    for i in range(hparts):
        over_y(i).start()

    for copy in load_small:
        copy.wait()
    wanted = targets_ref[...]
    lane = lax.broadcasted_iota(jnp.int32, (group, tokens), 1)
    members = member_ref[...].astype(jnp.float32)
    spread = jnp.zeros((group, tokens), jnp.float32)
    for e in range(members.shape[1]):
        spread = jnp.where(lane // seq == e, 1.0 - members[:, e : e + 1], spread)
    outs[0] = spread
    share_outs = pltpu.make_async_remote_copy(
        src_ref=outs.at[0],
        dst_ref=outs.at[1],
        send_sem=ou_send.at[0],
        recv_sem=ou_recv.at[0],
        device_id=(across, v),
        device_id_type=MESH,
    )
    share_outs.start()

    def product(which, block, j):
        words = heads[pl.ds(2 * block, 2), j].reshape(2 * head_rows, slab)
        where = pl.ds(pl.multiple_of(j * slab, slab), slab)
        return lax.dot_general(
            words,
            hid[which, :, where],
            (((1,), (1,)), ((), ())),
            preferred_element_type=jnp.float32,
        )

    def absorb(row0, logits, block):
        count = logits.shape[0]
        i = lax.broadcasted_iota(jnp.int32, (count, tokens), 0)
        first = (block + i // (2 * head_rows)) * 4 + y * 2 + i // head_rows % 2
        ids = (first * nv + v) * head_rows + i % head_rows
        hit = ids == wanted
        for s in range(logits.shape[1] // tokens):
            row = pl.ds(row0 + s, 1)
            mine = logits[:, s * tokens : (s + 1) * tokens]
            tgt[row] += jnp.sum(jnp.where(hit, mine, 0.0), axis=0, keepdims=True)
            others = jnp.where(hit, NEG_FILL, mine)
            before = top[row]
            raised = jnp.maximum(before, jnp.max(others, axis=0, keepdims=True))
            terms = jnp.sum(jnp.exp(others - raised), axis=0, keepdims=True)
            tot[row] = tot[row] * jnp.exp(before - raised) + terms
            top[row] = raised

    def fold_blocks(block, count, which, start, size):
        words = jnp.concatenate(
            [
                heads[pl.ds(2 * block, 2 * count), j].reshape(count * 2 * head_rows, slab)
                for j in range(chunks)
            ],
            axis=1,
        )
        logits = lax.dot_general(
            words,
            hid[which, pl.ds(start, size)],
            (((1,), (1,)), ((), ())),
            preferred_element_type=jnp.float32,
        )
        absorb(which * group + start // tokens, logits, block)

    def whole_block(which, block):
        fold_blocks(block, 1, which, 0, rows)

    def from_sibling(block):
        whole = heads.at[2 * block + 1 - c]
        pltpu.make_async_copy(whole, whole, sib_recv.at[block]).wait()

    def fold_step(k):
        @pl.when(z - k >= 0)
        def _():
            from_sibling(z - k)
            whole_block(0, z - k)

        @pl.when((k > 0) & (z + k < nz))
        def _():
            from_sibling(z + k)
            whole_block(0, z + k)

    def arrive(k, j):
        low, high = z - k, z + k

        @pl.when(low >= 0)
        def _():
            line(low, j, me).wait_recv()

            @pl.when(has_up)
            def _():
                line(low, j, me + 4).start()

            side(low, j, c).start()

        @pl.when(high < nz)
        def _():
            line(high, j, me).wait_recv()

            @pl.when(has_down)
            def _():
                line(high, j, me - 4).start()

            side(high, j, c).start()

    early = (last - 1) * chunks
    pace = max(1, min(2, early // hparts))

    def turn(r, _):
        arrive(1 + r // chunks, r % chunks)

        @pl.when((r % pace == pace - 1) & (r // pace < hparts))
        def _():
            i = r // pace
            over_y(i).wait_recv()
            for d in range(1, nv):
                over_x(d, i, v).start()

        @pl.when(r % chunks == 0)
        def _():
            fold_step(r // chunks)

        return 0

    lax.fori_loop(0, early, turn, 0)

    middle = chunks // 2
    by_piece = piece % tokens == 0
    unit = piece if by_piece else rows
    base = jnp.where(z == last, one, zero)
    acc[...] = jnp.zeros_like(acc)

    def closing(j, _):
        arrive(last, j)

        @pl.when(j == 0)
        def _():
            fold_step(last - 1)

        def catch_up(owner):
            start = pl.multiple_of(owner * unit, unit)
            fold_blocks(base, last, 1, start, unit)

            @pl.when(jnp.logical_not(at_end))
            def _():
                fold_blocks(last, 1, 1, start, unit)

        if by_piece:

            @pl.when(j == 0)
            def _():
                catch_up(v)

        @pl.when(j == middle)
        def _():
            for d in range(1, nv):
                theirs = pl.ds(pl.multiple_of((v + nv - d) % nv * piece, piece), piece)
                came = hid.at[1, theirs]
                pltpu.make_async_copy(came, came, hx_recv.at[d - 1]).wait()
                if by_piece:
                    catch_up((v + nv - d) % nv)
            if not by_piece:
                catch_up(zero)

            @pl.when(at_end)
            def _():
                def missed(i, _):
                    acc[1] += product(1, final, i)
                    return 0

                lax.fori_loop(0, middle - 1, missed, 0)

        @pl.when(at_end & (j >= 1))
        def _():
            side(final, j - 1, 1 - c).wait_recv()
            acc[0] += product(0, final, j - 1)

            @pl.when(j >= middle)
            def _():
                acc[1] += product(1, final, j - 1)

        return 0

    lax.fori_loop(0, chunks, closing, 0)

    @pl.when(at_end)
    def _():
        side(final, chunks - 1, 1 - c).wait_recv()
        for which in range(2):
            absorb(which * group, acc[which] + product(which, final, chunks - 1), final)

    stat_send[0] = top[...]
    stat_send[1] = tot[...]
    stat_send[2] = tgt[...]

    offsets = [(dy, d) for dy in range(2) for d in range(nv) if dy or d]

    def stats(dy, d):
        return pltpu.make_async_remote_copy(
            src_ref=stat_send,
            dst_ref=stat_recv.at[dy * nv + d],
            send_sem=st_send.at[0],
            recv_sem=st_recv.at[0],
            device_id=(across if dy else me, (v + d) % nv),
            device_id_type=MESH,
        )

    for dy, d in offsets:
        stats(dy, d).start()

    share_outs.wait_recv()
    outside = jnp.concatenate([outs[0], outs[1]], axis=0)

    def seen(slot, which):
        value = stat_recv[slot, which]
        return pltpu.roll(value, group, 0) if slot >= nv else value

    highest, summed, target_logit = top[...], tot[...], tgt[...]
    stat_all = stat_recv.at[pl.ds(1, 2 * nv - 1)]
    pltpu.make_async_copy(stat_all, stat_all, st_recv.at[0]).wait()
    for dy, d in offsets:
        slot = dy * nv + d
        theirs = seen(slot, 0)
        raised = jnp.maximum(highest, theirs)
        summed = summed * jnp.exp(highest - raised) + seen(slot, 1) * jnp.exp(theirs - raised)
        highest = raised
        target_logit = target_logit + seen(slot, 2)
    confidence = target_logit - (highest + jnp.log(summed))
    weighted = outside * confidence
    squared = weighted * confidence

    mom_send[0:1] = jnp.sum(weighted, axis=0, keepdims=True)
    mom_send[1:2] = jnp.sum(squared, axis=0, keepdims=True)

    around = [(dz, dc) for dz in range(nz) for dc in range(2) if dz or dc]

    def moments(dz, dc):
        column = (z + dz) % nz * 4 + y * 2 + (c + dc) % 2
        return pltpu.make_async_remote_copy(
            src_ref=mom_send,
            dst_ref=mom_recv.at[2 * dz + dc],
            send_sem=mo_send.at[0],
            recv_sem=mo_recv.at[0],
            device_id=(column, v),
            device_id_type=MESH,
        )

    for dz, dc in around:
        moments(dz, dc).start()
    total = mom_send[0:2]
    mom_all = mom_recv.at[pl.ds(1, 2 * nz - 1)]
    pltpu.make_async_copy(mom_all, mom_all, mo_recv.at[0]).wait()
    for dz, dc in around:
        total = total + mom_recv[2 * dz + dc, 0:2]
    first_moment, second_moment = total[0:1], total[1:2]
    out_count = (group * nsh) // 2 - outside
    out_mean = (first_moment - weighted) / out_count
    out_variance = (second_moment - squared) / out_count - out_mean * out_mean
    score = (confidence - out_mean) * lax.rsqrt(jnp.maximum(out_variance, 0.0) + VAR_FLOOR)
    keep = tokens // nv
    shifted = pltpu.roll(score, (nv - v) % nv * keep, 1)
    out_ref[...] = shifted[0:group, 0:keep]

    def drained(ref, sem):
        pltpu.make_async_copy(ref, ref, sem.at[0]).wait()

    @pl.when(at_end)
    def _():
        drained(heads.at[pl.ds(0, 1)], line_send)

    @pl.when(jnp.logical_not(at_end))
    def _():
        drained(heads.at[pl.ds(0, nz + 1)], line_send)

    drained(heads.at[pl.ds(0, nz)], sib_send)
    drained(hid.at[0, pl.ds(0, piece)], hy_send)
    drained(hid.at[0, pl.ds(0, (nv - 1) * piece)], hx_send)
    drained(stat_all, st_send)
    drained(mom_all, mo_send)
    share_outs.wait_send()


def per_device(nsh, nv, hidden, targets, membership, unembedding):
    group, tokens, width = hidden.shape
    head_rows = unembedding.shape[0]
    rows = group * tokens
    nz = nsh // 4
    chunks = HEAD_CHUNKS
    hparts = max(1, min(HIDDEN_CHUNKS, rows // nv // 16))
    dma = pltpu.SemaphoreType.DMA
    hbm, vmem = pl.BlockSpec(memory_space=pltpu.HBM), pl.BlockSpec(memory_space=pltpu.VMEM)
    return pl.pallas_call(
        functools.partial(kernel, nsh, nv, SEQ),
        out_shape=pltpu.VMEM((group, tokens // nv), jnp.float32),
        in_specs=[hbm] * 4,
        out_specs=vmem,
        scratch_shapes=[
            pltpu.VMEM((1, tokens), jnp.int32),
            pltpu.VMEM(membership.shape, jnp.int32),
            pltpu.VMEM((2, rows, width), jnp.bfloat16),
            pltpu.VMEM((2 * nz, chunks, head_rows, width // chunks), jnp.bfloat16),
            pltpu.VMEM((2 * group, tokens), jnp.float32),
            pltpu.VMEM((2 * group, tokens), jnp.float32),
            pltpu.VMEM((2 * group, tokens), jnp.float32),
            pltpu.VMEM((2, 2 * head_rows, rows), jnp.float32),
            pltpu.VMEM((2, group, tokens), jnp.float32),
            pltpu.VMEM((3, 2 * group, tokens), jnp.float32),
            pltpu.VMEM((2 * nv, 3, 2 * group, tokens), jnp.float32),
            pltpu.VMEM((8, tokens), jnp.float32),
            pltpu.VMEM((2 * nz, 8, tokens), jnp.float32),
            dma((chunks + 3,)),
            dma((1,)),
            dma((nz, chunks)),
            dma((1,)),
            dma((nz + chunks,)),
            dma((1,)),
            dma((hparts,)),
            dma((1,)),
            dma((max(1, nv - 1),)),
            dma((1,)),
            dma((1,)),
            dma((1,)),
            dma((1,)),
            dma((1,)),
            dma((1,)),
        ],
        compiler_params=pltpu.CompilerParams(
            collective_id=0, has_side_effects=True, vmem_limit_bytes=67035136
        ),
    )(hidden.reshape(rows, width), targets.reshape(1, tokens), membership, unembedding)


def solution(mesh):
    nsh, nv = mesh.shape["shadow"], mesh.shape["vocab"]
    return jax.shard_map(
        functools.partial(per_device, nsh, nv),
        mesh=mesh,
        in_specs=(P("shadow", None, None), P(), P("shadow", None), P(("shadow", "vocab"), None)),
        out_specs=P("shadow", "vocab"),
        check_vma=False,
    )
```

```python
import functools

import jax
import jax.numpy as jnp
from jax import lax
from jax.experimental import pallas as pl
from jax.experimental.pallas import tpu as pltpu
from jax.sharding import PartitionSpec as P

SEQ = 32
LANES = 128
NEG_FILL = -1e30
VAR_FLOOR = 0.5
MESH = pl.DeviceIdType.MESH

SLABS = 8
PIECES = ((0, 3), (3, 6), (6, 7), (7, 8))
HIDDEN_PARTS = 8


def kernel(
    nsh,
    nv,
    splits,
    seq,
    hidden_hbm,
    targets_hbm,
    member_hbm,
    head_hbm,
    out_ref,
    targets_ref,
    member_ref,
    want,
    hid,
    heads,
    top,
    tot,
    tgt,
    acc,
    outs,
    stat_send,
    stat_recv,
    mom_send,
    mom_recv,
    load_sem,
    line_send,
    line_recv,
    sib_send,
    sib_recv,
    hy_send,
    hy_recv,
    hx_send,
    hx_recv,
    hs_send,
    hs_recv,
    st_send,
    st_recv,
    mo_send,
    mo_recv,
    ou_send,
    ou_recv,
):
    nz = nsh // 4
    last = nz - 1
    slabs, head_rows, slab = heads.shape[1], heads.shape[2], heads.shape[3]
    rows = hid.shape[1]
    tokens = targets_ref.shape[1]
    group = rows // tokens
    piece = rows // nv
    hparts = hy_recv.shape[0]
    part = piece // hparts
    pieces = len(PIECES)
    sub = tokens // splits
    per_row = LANES // sub
    depth = group * sub // LANES
    strips = rows // LANES

    me = lax.axis_index("shadow")
    v = lax.axis_index("vocab")
    z, y, c = me // 4, (me // 2) % 2, me % 2
    far = 1 - y
    sibling = me + 1 - 2 * c
    across = me + 2 - 4 * y
    has_up, has_down = z + 1 < nz, z >= 1
    one, zero = jnp.int32(1), jnp.int32(0)
    at_end = (z == 0) | (z == last)
    final = jnp.where(z == 0, jnp.int32(last), zero)
    my_split = v if splits > 1 else zero

    load_head = [
        pltpu.make_async_copy(
            head_hbm.at[:, pl.ds(s * slab, slab)], heads.at[2 * z + c, s], load_sem.at[j]
        )
        for j, (a, b) in enumerate(PIECES)
        for s in range(a, b)
    ]
    load_hidden = [
        pltpu.make_async_copy(
            hidden_hbm.at[pl.ds(s * tokens + h * sub, sub)],
            hid.at[y, pl.ds((h * group + s) * sub, sub)],
            load_sem.at[pieces],
        )
        for h in range(splits)
        for s in range(group)
    ]
    load_small = [
        pltpu.make_async_copy(targets_hbm, targets_ref, load_sem.at[pieces + 1]),
        pltpu.make_async_copy(member_hbm, member_ref, load_sem.at[pieces + 2]),
    ]
    for copy in load_head + load_hidden + load_small:
        copy.start()

    barrier = pltpu.get_barrier_semaphore()

    def greet(s, w):
        pl.semaphore_signal(barrier, inc=1, device_id=(s, w), device_id_type=MESH)

    greet(sibling, v)
    greet(across, v)
    for d in range(1, nv):
        greet(me, (v + d) % nv)

    @pl.when(has_up)
    def _():
        greet(me + 4, v)

    @pl.when(has_down)
    def _():
        greet(me - 4, v)

    top[...] = jnp.full_like(top, NEG_FILL)
    tot[...] = jnp.zeros_like(tot)
    tgt[...] = jnp.zeros_like(tgt)
    pl.semaphore_wait(
        barrier, nv + 1 + jnp.where(has_up, one, zero) + jnp.where(has_down, one, zero)
    )

    def landed(ref, sem):
        pltpu.make_async_copy(ref, ref, sem).wait()

    def line(block, j, target):
        a, b = PIECES[j]
        where = heads.at[2 * block + c, pl.ds(a, b - a)]
        return pltpu.make_async_remote_copy(
            src_ref=where,
            dst_ref=where,
            send_sem=line_send.at[0],
            recv_sem=line_recv.at[block, j],
            device_id=(target, v),
            device_id_type=MESH,
        )

    def side(block, j):
        a, b = PIECES[j]
        where = heads.at[2 * block + c, pl.ds(a, b - a)]
        return pltpu.make_async_remote_copy(
            src_ref=where,
            dst_ref=where,
            send_sem=sib_send.at[0],
            recv_sem=sib_recv.at[block],
            device_id=(sibling, v),
            device_id_type=MESH,
        )

    def over_y(slot, i):
        where = pl.ds(pl.multiple_of(v * piece + i * part, part), part)
        return pltpu.make_async_remote_copy(
            src_ref=hid.at[slot, where],
            dst_ref=hid.at[slot, where],
            send_sem=hy_send.at[0],
            recv_sem=hy_recv.at[i],
            device_id=(across, v),
            device_id_type=MESH,
        )

    def over_x(d, i):
        where = pl.ds(pl.multiple_of(v * piece + i * part, part), part)
        return pltpu.make_async_remote_copy(
            src_ref=hid.at[far, where],
            dst_ref=hid.at[far, where],
            send_sem=hx_send.at[0],
            recv_sem=hx_recv.at[d - 1],
            device_id=(me, (v + d) % nv),
            device_id_type=MESH,
        )

    def to_sibling(slot, where, index):
        return pltpu.make_async_remote_copy(
            src_ref=hid.at[slot, where],
            dst_ref=hid.at[2 + slot, where],
            send_sem=hs_send.at[0],
            recv_sem=hs_recv.at[index],
            device_id=(sibling, v),
            device_id_type=MESH,
        )

    for j, (a, b) in enumerate(PIECES):
        landed(heads.at[2 * z + c, pl.ds(a, b - a)], load_sem.at[j])

        @pl.when(has_up)
        def _():
            line(z, j, me + 4).start()

        @pl.when(has_down)
        def _():
            line(z, j, me - 4).start()

        side(z, j).start()
    landed(hid.at[y], load_sem.at[pieces])
    for i in range(hparts):
        over_y(y, i).start()

    everything = pl.ds(0, rows)

    @pl.when(at_end)
    def _():
        to_sibling(y, everything, 0).start()

    for copy in load_small:
        copy.wait()
    lane = lax.broadcasted_iota(jnp.int32, (1, LANES), 1)
    ids_wanted = targets_ref[...]
    for q in range(strips):
        h = q // depth
        row = ids_wanted
        for k in range(per_row):
            moved = pltpu.roll(ids_wanted, (k - h) * sub % LANES, 1)
            row = jnp.where(lane // sub == k, moved, row)
        want[q : q + 1] = row
    members = member_ref[...].astype(jnp.float32)
    strip = lax.broadcasted_iota(jnp.int32, (depth, LANES), 0)
    place = lax.broadcasted_iota(jnp.int32, (depth, LANES), 1)
    shadow = strip * per_row + place // sub
    example = (my_split * sub + place % sub) // seq
    spread = jnp.zeros((depth, LANES), jnp.float32)
    for s in range(group):
        for e in range(members.shape[1]):
            spread = jnp.where(
                (shadow == s) & (example == e), 1.0 - members[s : s + 1, e : e + 1], spread
            )
    outs[y] = spread
    share_outs = pltpu.make_async_remote_copy(
        src_ref=outs.at[y],
        dst_ref=outs.at[y],
        send_sem=ou_send.at[0],
        recv_sem=ou_recv.at[0],
        device_id=(across, v),
        device_id_type=MESH,
    )
    share_outs.start()

    def absorb(row0, logits, ids):
        for s in range(logits.shape[1] // LANES):
            row = pl.ds(row0 + s, 1)
            hit = ids == want[pl.ds((row0 + s) % strips, 1)]
            mine = logits[:, s * LANES : (s + 1) * LANES]
            tgt[row] += jnp.sum(jnp.where(hit, mine, 0.0), axis=0, keepdims=True)
            others = jnp.where(hit, NEG_FILL, mine)
            before = top[row]
            raised = jnp.maximum(before, jnp.max(others, axis=0, keepdims=True))
            terms = jnp.sum(jnp.exp(others - raised), axis=0, keepdims=True)
            tot[row] = tot[row] * jnp.exp(before - raised) + terms
            top[row] = raised

    def columns(which, slot, where, a, b):
        return lax.dot_general(
            jnp.concatenate([which(s) for s in range(a, b)], axis=1),
            hid[slot, where, a * slab : b * slab],
            (((1,), (1,)), ((), ())),
            preferred_element_type=jnp.float32,
        )

    def fold_blocks(block, count, slot, start, size):
        height = count * 2 * head_rows

        def words(s):
            return heads[pl.ds(2 * block, 2 * count), s].reshape(height, slab)

        logits = columns(words, slot, pl.ds(start, size), 0, slabs)
        i = lax.broadcasted_iota(jnp.int32, (height, LANES), 0)
        first = (block + i // (2 * head_rows)) * 4 + y * 2 + i // head_rows % 2
        ids = (first * nv + v) * head_rows + i % head_rows
        absorb(slot * strips + start // LANES, logits, ids)

    def fold_own(block):
        landed(heads.at[2 * block + 1 - c], sib_recv.at[block])
        fold_blocks(block, 1, y, 0, rows)

    def fold_step(k):
        @pl.when(z - k >= 0)
        def _():
            fold_own(z - k)

        @pl.when((k > 0) & (z + k < nz))
        def _():
            fold_own(z + k)

    def arrive(k, j):
        low, high = z - k, z + k

        @pl.when(low >= 0)
        def _():
            line(low, j, me).wait_recv()

            @pl.when(has_up)
            def _():
                line(low, j, me + 4).start()

            side(low, j).start()

        @pl.when(high < nz)
        def _():
            line(high, j, me).wait_recv()

            @pl.when(has_down)
            def _():
                line(high, j, me - 4).start()

            side(high, j).start()

    early = (last - 1) * pieces
    pace = max(1, min(2, early // hparts))

    def turn(k, _):
        for j in range(pieces):
            r = (k - 1) * pieces + j
            arrive(k, j)

            @pl.when((r % pace == pace - 1) & (r // pace < hparts))
            def _():
                i = r // pace
                over_y(far, i).wait_recv()
                for d in range(1, nv):
                    over_x(d, i).start()

            if j == 0:
                fold_step(k - 1)
        return 0

    lax.fori_loop(1, last, turn, 0)

    by_piece = piece % LANES == 0
    unit = piece if by_piece else rows

    def other_piece(d):
        return pl.ds(pl.multiple_of((v + nv - d) % nv * piece, piece), piece)

    def from_x():
        for d in range(1, nv):
            landed(hid.at[far, other_piece(d)], hx_recv.at[d - 1])

    def catch_up(block, count, owner):
        start = pl.multiple_of(owner * unit, unit)
        fold_blocks(block, count, far, start, unit)

    def catch_rest(block, count):
        if by_piece:
            for d in range(1, nv):
                catch_up(block, count, (v + nv - d) % nv)
        else:
            catch_up(block, count, zero)

    @pl.when(jnp.logical_not(at_end))
    def _():
        fold_step(last - 1)
        if by_piece:
            catch_up(zero, nz, v)
        from_x()
        catch_rest(zero, nz)

    @pl.when(at_end)
    def _():
        base = jnp.where(z == last, one, zero)
        mine = pl.ds(pl.multiple_of(v * piece, piece), piece)
        to_sibling(far, mine, 1).start()
        fold_step(last - 1)
        if by_piece:
            catch_up(base, last, v)

        def words(s):
            return heads[2 * final + c, s]

        def came(j):
            line(final, j, me).wait_recv()

        def product(j, slot):
            return columns(words, slot, everything, *PIECES[j])

        came(0)
        landed(hid.at[2 + y], hs_recv.at[0])
        for slot in (y, 2 + y):
            acc[slot] = product(0, slot)
        from_x()
        for d in range(1, nv):
            to_sibling(far, other_piece(d), 1).start()
        catch_rest(base, last)
        landed(hid.at[2 + far], hs_recv.at[1])
        for slot in (far, 2 + far):
            acc[slot] = product(0, slot)
        for j in range(1, pieces - 1):
            came(j)
            for slot in range(4):
                acc[slot] += product(j, slot)
        came(pieces - 1)
        i = lax.broadcasted_iota(jnp.int32, (head_rows, LANES), 0)
        ids = ((final * 4 + y * 2 + c) * nv + v) * head_rows + i
        for slot in range(4):
            absorb(slot * strips, acc[slot] + product(pieces - 1, slot), ids)

    summed = tot[...]
    partial = jnp.where(summed > 0.0, top[...] + jnp.log(summed), NEG_FILL)
    for h in range(splits):
        for g in range(2):
            for w in range(2):
                a = (2 * g + w) * strips + h * depth
                stat_send[h, g, w * depth : (w + 1) * depth] = partial[a : a + depth]
                stat_send[h, g, (2 + w) * depth : (3 + w) * depth] = tgt[a : a + depth]

    mates = [
        (dc, dy, d) for dc in range(2) for dy in range(2) for d in range(nv) if dc or dy or d
    ]

    def stats(dc, dy, d):
        column = z * 4 + (y + dy) % 2 * 2 + (c + dc) % 2
        beside = (v + d) % nv
        return pltpu.make_async_remote_copy(
            src_ref=stat_send.at[beside if splits > 1 else 0, dc],
            dst_ref=stat_recv.at[(dc * 2 + dy) * nv + d],
            send_sem=st_send.at[0],
            recv_sem=st_recv.at[0],
            device_id=(column, beside),
            device_id_type=MESH,
        )

    for mate in mates:
        stats(*mate).start()

    share_outs.wait_recv()
    outside = jnp.concatenate([outs[0], outs[1]], axis=0)
    own = stat_send[my_split, 0]
    stat_all = stat_recv.at[pl.ds(1, 4 * nv - 1)]
    landed(stat_all, st_recv.at[0])
    parts = [own] + [stat_recv[(dc * 2 + dy) * nv + d] for dc, dy, d in mates]
    highest = functools.reduce(jnp.maximum, [p[0 : 2 * depth] for p in parts])
    summed = sum(jnp.exp(p[0 : 2 * depth] - highest) for p in parts)
    target_logit = sum(p[2 * depth : 4 * depth] for p in parts)
    confidence = target_logit - (highest + jnp.log(summed))
    weighted = outside * confidence
    squared = weighted * confidence

    mom_send[0:1] = jnp.sum(weighted, axis=0, keepdims=True)
    mom_send[1:2] = jnp.sum(squared, axis=0, keepdims=True)

    around = [(dz, dc) for dz in range(nz) for dc in range(2) if dz or dc]

    def moments(dz, dc):
        column = (z + dz) % nz * 4 + y * 2 + (c + dc) % 2
        return pltpu.make_async_remote_copy(
            src_ref=mom_send,
            dst_ref=mom_recv.at[2 * dz + dc],
            send_sem=mo_send.at[0],
            recv_sem=mo_recv.at[0],
            device_id=(column, v),
            device_id_type=MESH,
        )

    for dz, dc in around:
        moments(dz, dc).start()
    total = mom_send[0:2]
    mom_all = mom_recv.at[pl.ds(1, 2 * nz - 1)]
    landed(mom_all, mo_recv.at[0])
    for dz, dc in around:
        total = total + mom_recv[2 * dz + dc, 0:2]
    total = sum(pltpu.roll(total, k * sub, 1) if k else total for k in range(per_row))
    first_moment, second_moment = total[0:1], total[1:2]
    out_count = (group * nsh) // 2 - outside
    out_mean = (first_moment - weighted) / out_count
    out_variance = (second_moment - squared) / out_count - out_mean * out_mean
    score = (confidence - out_mean) * lax.rsqrt(jnp.maximum(out_variance, 0.0) + VAR_FLOOR)
    score = jnp.where(y == 0, score[0:depth], score[depth : 2 * depth])
    keep = tokens // nv
    if splits > 1:
        for s in range(group):
            p, a = s // per_row, s % per_row * sub
            out_ref[s : s + 1] = score[p : p + 1, a : a + sub]
    else:
        shifted = pltpu.roll(score, (nv - v) % nv * keep, 1)
        out_ref[...] = shifted[0:group, 0:keep]

    @pl.when(at_end)
    def _():
        landed(heads.at[pl.ds(0, 1)], line_send.at[0])
        landed(heads.at[pl.ds(0, nz - 1)], sib_send.at[0])
        landed(hid.at[pl.ds(0, 2)], hs_send.at[0])

    @pl.when(jnp.logical_not(at_end))
    def _():
        landed(heads.at[pl.ds(0, nz + 1)], line_send.at[0])
        landed(heads.at[pl.ds(0, nz)], sib_send.at[0])

    landed(hid.at[0, pl.ds(0, piece)], hy_send.at[0])
    landed(hid.at[0, pl.ds(0, (nv - 1) * piece)], hx_send.at[0])
    landed(stat_all, st_send.at[0])
    landed(mom_all, mo_send.at[0])
    share_outs.wait_send()


def per_device(nsh, nv, hidden, targets, membership, unembedding):
    group, tokens, width = hidden.shape
    head_rows = unembedding.shape[0]
    rows = group * tokens
    nz = nsh // 4
    pieces = len(PIECES)
    splits = nv if rows // nv % (2 * LANES) == 0 else 1
    depth = rows // splits // LANES
    hparts = max(1, min(HIDDEN_PARTS, rows // nv // 16, (nz - 2) * pieces))
    dma = pltpu.SemaphoreType.DMA
    hbm, vmem = pl.BlockSpec(memory_space=pltpu.HBM), pl.BlockSpec(memory_space=pltpu.VMEM)
    strips = 4 * rows // LANES
    return pl.pallas_call(
        functools.partial(kernel, nsh, nv, splits, SEQ),
        out_shape=pltpu.VMEM((group, tokens // nv), jnp.float32),
        in_specs=[hbm] * 4,
        out_specs=vmem,
        scratch_shapes=[
            pltpu.VMEM((1, tokens), jnp.int32),
            pltpu.VMEM(membership.shape, jnp.int32),
            pltpu.VMEM((rows // LANES, LANES), jnp.int32),
            pltpu.VMEM((4, rows, width), jnp.bfloat16),
            pltpu.VMEM((2 * nz, SLABS, head_rows, width // SLABS), jnp.bfloat16),
            pltpu.VMEM((strips, LANES), jnp.float32),
            pltpu.VMEM((strips, LANES), jnp.float32),
            pltpu.VMEM((strips, LANES), jnp.float32),
            pltpu.VMEM((4, head_rows, rows), jnp.float32),
            pltpu.VMEM((2, depth, LANES), jnp.float32),
            pltpu.VMEM((splits, 2, 4 * depth, LANES), jnp.float32),
            pltpu.VMEM((4 * nv, 4 * depth, LANES), jnp.float32),
            pltpu.VMEM((8, LANES), jnp.float32),
            pltpu.VMEM((2 * nz, 8, LANES), jnp.float32),
            dma((pieces + 3,)),
            dma((1,)),
            dma((nz, pieces)),
            dma((1,)),
            dma((nz,)),
            dma((1,)),
            dma((hparts,)),
            dma((1,)),
            dma((max(1, nv - 1),)),
            dma((1,)),
            dma((2,)),
            dma((1,)),
            dma((1,)),
            dma((1,)),
            dma((1,)),
            dma((1,)),
            dma((1,)),
        ],
        compiler_params=pltpu.CompilerParams(
            collective_id=0, has_side_effects=True, vmem_limit_bytes=67035136
        ),
    )(hidden.reshape(rows, width), targets.reshape(1, tokens), membership, unembedding)


def solution(mesh):
    nsh, nv = mesh.shape["shadow"], mesh.shape["vocab"]
    return jax.shard_map(
        functools.partial(per_device, nsh, nv),
        mesh=mesh,
        in_specs=(P("shadow", None, None), P(), P("shadow", None), P(("shadow", "vocab"), None)),
        out_specs=P("shadow", "vocab"),
        check_vma=False,
    )
```
